32 devices in a mesh: tm: 4 (over x, core), env: 8 (over z, y).
Axes of the slice: x: 2, y: 2, z: 4, core: 2. Of those that a mesh axis runs over, the one named last changes fastest.
Arguments:
- rewards: float32 [2048, 4096], P('tm', 'env'), may hold values from -0.4 to 0.4
- values: float32 [2048, 4096], P('tm', 'env'), may hold values from -0.4 to 0.4
- done_flags: int32 [2048, 4096], P('tm', 'env'), may hold values 0 or 1
- bootstrap: float32 [4096], P('env'), may hold values from -0.4 to 0.4
- discount_horizon: float32 [4096], P('env'), may hold values from 10 to 16384
- trace_horizon: float32 [4096], P('env'), may hold values from 10 to 16384
Outputs:
- norm_advantage: float32 [2048, 4096], P('tm', 'env')
- return_target: float32 [2048, 4096], P('tm', 'env')
The draws below stay inside these ranges and needn't reach their ends.
All inputs are finite; a program needn't handle non-finite values. No bound on the sum of `done_flags` on one device may be relied on, other than what follows from the above.
Results may differ from the reference program's by a relative error of at most 0.0003.
Values sent between devices are 32-bit elements; how exact they have to be, the bound alone decides.
No kernel may reach another device: no remote copies, remote signals or barrier semaphores. Data moves between devices by JAX's collectives and lax.ppermute only.
A program may use at most 64 MiB of HBM per device.

```python
import jax
import jax.numpy as jnp
from jax import lax

STEPS = 2048
ENVS = 4096


def short_flags(key):
    flag_key = jax.random.fold_in(key, 5)
    share_key, pick_key = jax.random.split(flag_key)
    share_short = jax.random.uniform(share_key, (), jnp.float32, 0.35, 0.65)
    return jax.random.uniform(pick_key, (ENVS,), jnp.float32) < share_short


def horizon_values(key, salt):
    flags = short_flags(key)
    own_key = jax.random.fold_in(key, salt)
    short_key, long_key = jax.random.split(own_key)
    short_value = jnp.exp(jax.random.uniform(short_key, (ENVS,), jnp.float32, jnp.log(10.0), jnp.log(40.0)))
    long_value = jnp.exp(jax.random.uniform(long_key, (ENVS,), jnp.float32, jnp.log(2.0 * STEPS), jnp.log(8.0 * STEPS)))
    picked = jnp.where(flags, short_value, long_value)
    return jnp.clip(picked, 10.0, 8.0 * STEPS).astype(jnp.float32)


def draw_discount_horizon(key, part):
    return horizon_values(key, 11)


def draw_trace_horizon(key, part):
    return horizon_values(key, 23)


def plant(result, rng, smallest, largest):
    dims = result.shape
    index_at = [jax.random.randint(jax.random.fold_in(rng, axis), (), 0, dims[axis]) for axis in range(len(dims))]
    result = result.at[tuple(index_at)].set(smallest)
    longest = dims.index(max(dims))
    index_at[longest] = (index_at[longest] + 1) % dims[longest]
    return result.at[tuple(index_at)].set(largest)


def block_levels(key, dims, pieces, low, top_value):
    level, own = 1.0, jax.random.fold_in(key, 6)
    for axis_at, parts in pieces:
        heights = jnp.exp(jax.random.uniform(jax.random.fold_in(own, axis_at), (parts,), jnp.float32, low / len(pieces), top_value / len(pieces)))
        level = level * jnp.repeat(heights, dims[axis_at] // parts).reshape([-1 if axis == axis_at else 1 for axis in range(len(dims))])
    return level


def gaussian(rng, dims, spread, most, shards=(), dtype=jnp.bfloat16):
    loudness = block_levels(rng, dims, shards, -0.22, 0.18) if shards else 1.0
    drawn = jax.random.normal(rng, dims, jnp.float32) * spread * loudness
    return jnp.minimum(jnp.maximum(drawn, -most), most).astype(dtype)


def setup_inputs(seed: int = 0) -> dict:
    seeds = jax.random.split(jax.random.key(seed), 7)
    return {
        "rewards": gaussian(seeds[0], (STEPS, ENVS), 0.05, 0.4, ((0, 4), (1, 8)), jnp.float32),
        "values": gaussian(seeds[1], (STEPS, ENVS), 0.05, 0.4, ((0, 4), (1, 8)), jnp.float32),
        "done_flags": plant((jax.random.randint(seeds[2], (STEPS, ENVS), 0, 2 * STEPS) < 1).astype(jnp.int32), jax.random.fold_in(seeds[2], 1), 0, 1),
        "bootstrap": gaussian(seeds[3], (ENVS,), 0.05, 0.4, ((0, 8),), jnp.float32),
        "discount_horizon": draw_discount_horizon(jax.random.fold_in(seeds[6], 71), 0),
        "trace_horizon": draw_trace_horizon(jax.random.fold_in(seeds[6], 71), 0),
    }


def reference(rewards, values, done_flags, bootstrap, discount_horizon, trace_horizon):
    discount = 1.0 - 1.0 / discount_horizon
    trace_decay = 1.0 - 1.0 / trace_horizon
    keep_mask = 1.0 - done_flags.astype(jnp.float32)
    next_value = jnp.concatenate([values[1:], bootstrap[None, :]], axis=0)
    step_error = rewards + discount[None, :] * next_value * keep_mask - values
    carry_rate = (discount * trace_decay)[None, :] * keep_mask

    def stepper(carry_in, row):
        rate_row, error_row = row
        gain_row = error_row + rate_row * carry_in
        return (gain_row, gain_row)
    start_carry = jnp.zeros_like(bootstrap)
    _, advantage = lax.scan(stepper, start_carry, (carry_rate, step_error), reverse=True)
    cell_count = 1.0 * advantage.size
    mean_value = jnp.sum(advantage) / cell_count
    variance = jnp.sum((advantage - mean_value) ** 2) / cell_count
    norm_advantage = (advantage - mean_value) / jnp.sqrt(variance + 1.0)
    return_target = advantage + values
    return (norm_advantage, return_target)
```

```python
import functools

import jax
import jax.numpy as jnp
from jax import lax
from jax.experimental import pallas as pl
from jax.experimental.pallas import tpu as pltpu
from jax.sharding import PartitionSpec as P

LANES = 128
SUBS = 8
F32 = jnp.float32


def spread(row):
    return jnp.broadcast_to(row, (SUBS, row.shape[1]))


def scan_kernel(r_ref, v_ref, d_ref, dh_ref, th_ref, g_ref, p_ref, tot_ref, carry, acc):
    step = pl.program_id(0)
    rows, width = r_ref.shape

    @pl.when(step == 0)
    def _():
        carry[0] = jnp.zeros((SUBS, width), F32)
        carry[1] = jnp.ones((SUBS, width), F32)
        acc[...] = jnp.zeros(acc.shape, F32)

    sub = lax.broadcasted_iota(jnp.int32, (SUBS, LANES), 0)
    masks = {k: sub < SUBS - k for k in (1, 2, 4)}
    for c in range(width // LANES):
        at = pl.ds(c * LANES, LANES)
        trace = 1.0 - 1.0 / th_ref[:, at]
        rate = (1.0 - 1.0 / dh_ref[:, at]) * trace
        inv = 1.0 / trace
        rate, inv, extra = spread(rate), spread(inv), spread(inv - 1.0)
        z_in, p_in = carry[0, :, at], carry[1, :, at]
        sums = [acc[i, :, at] for i in range(5)]
        for j in reversed(range(rows // SUBS)):
            rs = pl.ds(j * SUBS, SUBS)
            v = v_ref[rs, at]
            u = r_ref[rs, at] + v * extra
            a = jnp.where(d_ref[rs, at] != 0, 0.0, rate)
            for k in (1, 2, 4):
                m = masks[k]
                u = u + jnp.where(m, a, 0.0) * pltpu.roll(u, SUBS - k, 0)
                a = a * jnp.where(m, pltpu.roll(a, SUBS - k, 0), 1.0)
            g = u + a * z_in - v * inv
            p = a * p_in
            z_in = spread(u[0:1]) + spread(a[0:1]) * z_in
            p_in = spread(a[0:1]) * p_in
            g_ref[rs, at] = g
            p_ref[rs, at] = p
            sums = [sums[0] + p, sums[1] + g * p, sums[2] + p * p, sums[3] + g, sums[4] + g * g]
        carry[0, :, at] = z_in
        carry[1, :, at] = p_in
        for i in range(5):
            acc[i, :, at] = sums[i]

    @pl.when(step == pl.num_programs(0) - 1)
    def _():
        tot_ref[0:1] = carry[1, 0:1]
        tot_ref[1:2] = carry[0, 0:1]
        for i in range(5):
            tot_ref[2 + i:3 + i] = jnp.sum(acc[i], axis=0, keepdims=True)
        tot_ref[7:8] = jnp.zeros((1, width), F32)


def pair_kernel(at_ref, mine_ref, other_ref, boot_ref, th_ref, send_ref, aux_ref, *, slots, copies):
    width = mine_ref.shape[1]
    half = width // 2
    m = half // LANES
    odd, last = at_ref[0], at_ref[1]
    late_here = odd == 1
    mine, other = mine_ref[...], other_ref[...]
    late = jnp.where(late_here, mine, other)
    early = jnp.where(late_here, other, mine)
    la, lz, lp, lgp, lpp, lg, lgg = [late[i:i + 1] for i in range(7)]
    ea, ez, ep, egp, epp, eg, egg = [early[i:i + 1] for i in range(7)]
    a, z = la * ea, ez + ea * lz
    p = lp + ep * la
    gp = lgp + (egp + epp * lz) * la
    pp = lpp + epp * la * la
    g = lg + eg + ep * lz
    gg = lgg + egg + (2.0 * egp + epp * lz) * lz
    known = boot_ref[...] / (1.0 - 1.0 / th_ref[...])
    is_last = last == 1
    g_end = g + p * known
    gg_end = gg + (2.0 * gp + pp * known) * known
    z_end = z + a * known
    g = jnp.where(is_last, g_end, g)
    gg = jnp.where(is_last, gg_end, gg)
    if slots == 3:
        parts = [jnp.where(is_last, z_end, p), gp, pp]
    else:
        parts = [jnp.where(is_last, z_end, z), p, gp, pp, a]
    mult = jnp.where(late_here, jnp.ones_like(la), la)
    add = jnp.where(late_here, jnp.zeros_like(la), lz)
    aux_ref[0:1] = jnp.where(is_last, 0.0, mult)
    aux_ref[1:2] = jnp.where(is_last, add + mult * known, add)
    aux_ref[2:8] = jnp.zeros((6, width), F32)

    def own(x):
        return jnp.where(late_here, x[:, half:], x[:, :half])

    rows = []
    for part in parts:
        h = own(part)
        rows += [h[:, i * LANES:(i + 1) * LANES] for i in range(m)]
    for total in (g, gg):
        h = own(total)
        rows.append(sum(h[:, i * LANES:(i + 1) * LANES] for i in range(m)))
    block = jnp.concatenate(rows, axis=0)
    send_ref[...] = jnp.broadcast_to(block[None], (copies,) + block.shape)


def finish_kernel(at_ref, got_ref, aux_ref, v_ref, g_ref, p_ref, norm_ref, ret_ref, z_ref, st_ref,
                  *, slots, pairs, groups, cells):
    rows, width = v_ref.shape
    half = width // 2
    m = half // LANES

    @pl.when(pl.program_id(0) == 0)
    def _():
        pair, group = at_ref[2], at_ref[3]
        n = 2 * groups
        base = slots * m
        got = [got_ref[k * n:(k + 1) * n] for k in range(pairs)]
        s1 = sum(jnp.sum(x[:, base:base + 1], axis=0) for x in got)
        s2 = sum(jnp.sum(x[:, base + 1:base + 2], axis=0) for x in got)
        off = 0 if slots == 3 else m
        z = got[pairs - 1][:, 0:m]
        here = [got_ref[(pairs - 1) * n + core * groups + group, 0:m] for core in range(2)]
        pick = here
        for k in reversed(range(pairs - 1)):
            x = got[k]
            p, gp, pp = [x[:, off + i * m:off + (i + 1) * m] for i in range(3)]
            t1 = jnp.sum(p * z, axis=0)
            t2 = jnp.sum((2.0 * gp + pp * z) * z, axis=0)
            s1 = s1 + jnp.sum(t1, axis=0, keepdims=True)
            s2 = s2 + jnp.sum(t2, axis=0, keepdims=True)
            pick = [jnp.where(pair == k, b, a) for a, b in zip(pick, here)]
            if k:
                z = x[:, 0:m] + x[:, 4 * m:5 * m] * z
                nxt = [got_ref[k * n + core * groups + group] for core in range(2)]
                here = [y[0:m] + y[4 * m:5 * m] * h for y, h in zip(nxt, here)]
        flat = jnp.concatenate([h[i:i + 1] for h in pick for i in range(m)], axis=1)
        z_in = aux_ref[1:2] + aux_ref[0:1] * flat
        mean = jnp.sum(s1, axis=1, keepdims=True) / cells
        var = jnp.sum(s2, axis=1, keepdims=True) / cells - mean * mean
        scale = 1.0 / jnp.sqrt(var + 1.0)
        z_ref[...] = spread(z_in)
        st_ref[0] = jnp.broadcast_to(mean, (SUBS, LANES))
        st_ref[1] = jnp.broadcast_to(scale, (SUBS, LANES))

    mean, scale = st_ref[0], st_ref[1]
    for c in range(width // LANES):
        at = pl.ds(c * LANES, LANES)
        z_in = z_ref[:, at]
        for j in range(rows // SUBS):
            rs = pl.ds(j * SUBS, SUBS)
            adv = g_ref[rs, at] + p_ref[rs, at] * z_in
            norm_ref[rs, at] = (adv - mean) * scale
            ret_ref[rs, at] = adv + v_ref[rs, at]


def local(rewards, values, done_flags, bootstrap, discount_horizon, trace_horizon):
    rows, width = rewards.shape
    blocks, groups = lax.axis_size("tm"), lax.axis_size("env")
    pairs, devices = blocks // 2, blocks * groups
    slots = 3 if pairs == 2 else 5
    m = width // 2 // LANES
    block_at, group = lax.axis_index("tm"), lax.axis_index("env")
    place = jnp.stack([block_at % 2, (block_at // 2 == pairs - 1).astype(jnp.int32), block_at // 2, group]).astype(jnp.int32)
    boot, dh, th = bootstrap[None], discount_horizon[None], trace_horizon[None]

    steps = 4
    part = rows // steps
    back = pl.BlockSpec((part, width), lambda i: (steps - 1 - i, 0))
    fore = pl.BlockSpec((part, width), lambda i: (i, 0))
    row = pl.BlockSpec((1, width), lambda i: (0, 0))
    eight = pl.BlockSpec((SUBS, width), lambda i: (0, 0))
    full = jax.ShapeDtypeStruct((rows, width), F32)
    gain, weight, totals = pl.pallas_call(
        scan_kernel,
        grid=(steps,),
        in_specs=[back, back, back, row, row],
        out_specs=[back, back, eight],
        out_shape=[full, full, jax.ShapeDtypeStruct((SUBS, width), F32)],
        scratch_shapes=[pltpu.VMEM((2, SUBS, width), F32), pltpu.VMEM((5, SUBS, width), F32)],
        name="scan",
    )(rewards, values, done_flags, dh, th)

    other = lax.ppermute(totals, "tm", [(i, i ^ 1) for i in range(blocks)])
    packed = slots * m + 2
    vmem = pl.BlockSpec(memory_space=pltpu.VMEM)
    smem = pl.BlockSpec(memory_space=pltpu.SMEM)
    send, aux = pl.pallas_call(
        functools.partial(pair_kernel, slots=slots, copies=devices),
        in_specs=[smem, vmem, vmem, vmem, vmem],
        out_specs=[vmem, vmem],
        out_shape=[jax.ShapeDtypeStruct((devices, packed, LANES), F32), jax.ShapeDtypeStruct((SUBS, width), F32)],
        name="pair",
    )(place, totals, other, boot, th)
    got = lax.all_to_all(send, ("tm", "env"), 0, 0, tiled=True)

    whole = pl.BlockSpec((devices, packed, LANES), lambda i: (0, 0, 0))
    return tuple(pl.pallas_call(
        functools.partial(finish_kernel, slots=slots, pairs=pairs, groups=groups,
                          cells=1.0 * rows * width * devices),
        grid=(steps,),
        in_specs=[smem, whole, eight, fore, fore, fore],
        out_specs=[fore, fore],
        out_shape=[full, full],
        scratch_shapes=[pltpu.VMEM((SUBS, width), F32), pltpu.VMEM((2, SUBS, LANES), F32)],
        name="finish",
    )(place, got, aux, values, gain, weight))


def solution(mesh):
    placed = (P("tm", "env"), P("tm", "env"), P("tm", "env"), P("env"), P("env"), P("env"))
    return jax.shard_map(
        local,
        mesh=mesh,
        in_specs=placed,
        out_specs=(P("tm", "env"), P("tm", "env")),
        check_vma=False,
    )
```

```python
import functools

import jax
import jax.numpy as jnp
from jax import lax
from jax.experimental import pallas as pl
from jax.experimental.pallas import tpu as pltpu
from jax.sharding import PartitionSpec as P

LANES = 128
SUBS = 8
F32 = jnp.float32


def spread(row):
    return jnp.broadcast_to(row, (SUBS, row.shape[1]))


def scan_kernel(r_ref, v_ref, d_ref, boot_ref, dh_ref, th_ref, g_ref, p_ref, h_ref, tot_ref, carry, acc):
    step = pl.program_id(0)
    rows, width = r_ref.shape
    first = (pl.num_programs(0) - 1 - step) * rows

    @pl.when(step == 0)
    def _():
        carry[0] = jnp.zeros((SUBS, width), F32)
        carry[1] = jnp.ones((SUBS, width), F32)
        acc[...] = jnp.zeros(acc.shape, F32)

    sub = lax.broadcasted_iota(jnp.int32, (SUBS, LANES), 0)
    masks = {k: sub < SUBS - k for k in (1, 2, 4)}
    for c in range(width // LANES):
        at = pl.ds(c * LANES, LANES)
        trace = 1.0 - 1.0 / th_ref[:, at]
        rate = (1.0 - 1.0 / dh_ref[:, at]) * trace
        inv = 1.0 / trace
        rate, inv, extra = spread(rate), spread(inv), spread(inv - 1.0)
        z_in, p_in = carry[0, :, at], carry[1, :, at]
        sums = [acc[i, :, at] for i in range(5)]
        for j in reversed(range(rows // SUBS)):
            rs = pl.ds(j * SUBS, SUBS)
            v = v_ref[rs, at]
            u = r_ref[rs, at] + v * extra
            a = jnp.where(d_ref[rs, at] != 0, 0.0, rate)
            for k in (1, 2, 4):
                m = masks[k]
                u = u + jnp.where(m, a, 0.0) * pltpu.roll(u, SUBS - k, 0)
                a = a * jnp.where(m, pltpu.roll(a, SUBS - k, 0), 1.0)
            g = u + a * z_in - v * inv
            p = a * p_in
            z_in = spread(u[0:1]) + spread(a[0:1]) * z_in
            p_in = spread(a[0:1]) * p_in
            to = pl.ds(pl.multiple_of(first + j * SUBS, SUBS), SUBS)
            g_ref[to, at] = g
            p_ref[to, at] = p
            h_ref[to, at] = g + v
            sums = [sums[0] + p, sums[1] + g * p, sums[2] + p * p, sums[3] + g, sums[4] + g * g]
        carry[0, :, at] = z_in
        carry[1, :, at] = p_in
        for i in range(5):
            acc[i, :, at] = sums[i]

    @pl.when(step == pl.num_programs(0) - 1)
    def _():
        tot_ref[0:1] = carry[1, 0:1]
        tot_ref[1:2] = carry[0, 0:1]
        for i in range(5):
            tot_ref[2 + i:3 + i] = jnp.sum(acc[i], axis=0, keepdims=True)
        tot_ref[7:8] = boot_ref[...] / (1.0 - 1.0 / th_ref[...])


def pair_kernel(at_ref, mine_ref, other_ref, send_ref, aux_ref, *, slots, copies):
    width = mine_ref.shape[1]
    half = width // 2
    m = half // LANES
    odd, last = at_ref[0], at_ref[1]
    late_here = odd == 1
    mine, other = mine_ref[...], other_ref[...]
    late = jnp.where(late_here, mine, other)
    early = jnp.where(late_here, other, mine)
    la, lz, lp, lgp, lpp, lg, lgg = [late[i:i + 1] for i in range(7)]
    ea, ez, ep, egp, epp, eg, egg = [early[i:i + 1] for i in range(7)]
    a, z = la * ea, ez + ea * lz
    p = lp + ep * la
    gp = lgp + (egp + epp * lz) * la
    pp = lpp + epp * la * la
    g = lg + eg + ep * lz
    gg = lgg + egg + (2.0 * egp + epp * lz) * lz
    known = mine[7:8]
    is_last = last == 1
    g_end = g + p * known
    gg_end = gg + (2.0 * gp + pp * known) * known
    z_end = z + a * known
    g = jnp.where(is_last, g_end, g)
    gg = jnp.where(is_last, gg_end, gg)
    if slots == 3:
        parts = [jnp.where(is_last, z_end, p), gp, pp]
    else:
        parts = [jnp.where(is_last, z_end, z), p, gp, pp, a]
    mult = jnp.where(late_here, jnp.ones_like(la), la)
    add = jnp.where(late_here, jnp.zeros_like(la), lz)
    aux_ref[0:1] = jnp.where(is_last, 0.0, mult)
    aux_ref[1:2] = jnp.where(is_last, add + mult * known, add)
    aux_ref[2:8] = jnp.zeros((6, width), F32)

    def own(x):
        return jnp.where(late_here, x[:, half:], x[:, :half])

    rows = []
    for part in parts:
        h = own(part)
        rows += [h[:, i * LANES:(i + 1) * LANES] for i in range(m)]
    for total in (g, gg):
        h = own(total)
        rows.append(sum(h[:, i * LANES:(i + 1) * LANES] for i in range(m)))
    block = jnp.concatenate(rows, axis=0)
    send_ref[...] = jnp.broadcast_to(block[None], (copies,) + block.shape)


def finish_kernel(at_ref, got_ref, aux_ref, h_ref, g_ref, p_ref, norm_ref, ret_ref, z_ref, st_ref,
                  *, slots, pairs, groups, cells):
    rows, width = norm_ref.shape
    first = pl.program_id(0) * rows
    half = width // 2
    m = half // LANES

    @pl.when(pl.program_id(0) == 0)
    def _():
        pair, group = at_ref[2], at_ref[3]
        n = 2 * groups
        base = slots * m
        got = [got_ref[k * n:(k + 1) * n] for k in range(pairs)]
        s1 = sum(jnp.sum(x[:, base:base + 1], axis=0) for x in got)
        s2 = sum(jnp.sum(x[:, base + 1:base + 2], axis=0) for x in got)
        off = 0 if slots == 3 else m
        z = got[pairs - 1][:, 0:m]
        here = [got_ref[(pairs - 1) * n + core * groups + group, 0:m] for core in range(2)]
        pick = here
        for k in reversed(range(pairs - 1)):
            x = got[k]
            p, gp, pp = [x[:, off + i * m:off + (i + 1) * m] for i in range(3)]
            t1 = jnp.sum(p * z, axis=0)
            t2 = jnp.sum((2.0 * gp + pp * z) * z, axis=0)
            s1 = s1 + jnp.sum(t1, axis=0, keepdims=True)
            s2 = s2 + jnp.sum(t2, axis=0, keepdims=True)
            pick = [jnp.where(pair == k, b, a) for a, b in zip(pick, here)]
            if k:
                z = x[:, 0:m] + x[:, 4 * m:5 * m] * z
                nxt = [got_ref[k * n + core * groups + group] for core in range(2)]
                here = [y[0:m] + y[4 * m:5 * m] * h for y, h in zip(nxt, here)]
        flat = jnp.concatenate([h[i:i + 1] for h in pick for i in range(m)], axis=1)
        z_in = aux_ref[1:2] + aux_ref[0:1] * flat
        mean = jnp.sum(s1, axis=1, keepdims=True) / cells
        var = jnp.sum(s2, axis=1, keepdims=True) / cells - mean * mean
        scale = 1.0 / jnp.sqrt(var + 1.0)
        z_ref[...] = spread(z_in)
        st_ref[0] = jnp.broadcast_to(mean, (SUBS, LANES))
        st_ref[1] = jnp.broadcast_to(scale, (SUBS, LANES))

    mean, scale = st_ref[0], st_ref[1]
    for c in range(width // LANES):
        at = pl.ds(c * LANES, LANES)
        z_in = z_ref[:, at]
        for j in range(rows // SUBS):
            rs = pl.ds(j * SUBS, SUBS)
            of = pl.ds(pl.multiple_of(first + j * SUBS, SUBS), SUBS)
            lift = p_ref[of, at] * z_in
            norm_ref[rs, at] = (g_ref[of, at] + lift - mean) * scale
            ret_ref[rs, at] = h_ref[of, at] + lift


def local(rewards, values, done_flags, bootstrap, discount_horizon, trace_horizon):
    rows, width = rewards.shape
    blocks, groups = lax.axis_size("tm"), lax.axis_size("env")
    pairs, devices = blocks // 2, blocks * groups
    slots = 3 if pairs == 2 else 5
    m = width // 2 // LANES
    block_at, group = lax.axis_index("tm"), lax.axis_index("env")
    place = jnp.stack([block_at % 2, (block_at // 2 == pairs - 1).astype(jnp.int32), block_at // 2, group]).astype(jnp.int32)
    boot, dh, th = bootstrap[None], discount_horizon[None], trace_horizon[None]

    steps = 4
    part = rows // steps
    back = pl.BlockSpec((part, width), lambda i: (steps - 1 - i, 0))
    fore = pl.BlockSpec((part, width), lambda i: (i, 0))
    row = pl.BlockSpec((1, width), lambda i: (0, 0))
    eight = pl.BlockSpec((SUBS, width), lambda i: (0, 0))
    full = jax.ShapeDtypeStruct((rows, width), F32)
    vmem = pl.BlockSpec(memory_space=pltpu.VMEM)
    smem = pl.BlockSpec(memory_space=pltpu.SMEM)
    small = pltpu.CompilerParams(vmem_limit_bytes=16 << 20)
    gain, weight, level, totals = pl.pallas_call(
        scan_kernel,
        grid=(steps,),
        in_specs=[back, back, back, row, row, row],
        out_specs=[vmem, vmem, vmem, eight],
        out_shape=[full, full, full, jax.ShapeDtypeStruct((SUBS, width), F32)],
        scratch_shapes=[pltpu.VMEM((2, SUBS, width), F32), pltpu.VMEM((5, SUBS, width), F32)],
        compiler_params=small,
        name="scan",
    )(*(pltpu.with_memory_space_constraint(x, pltpu.HBM) for x in (rewards, values, done_flags, boot, dh, th)))

    other = lax.ppermute(totals, "tm", [(i, i ^ 1) for i in range(blocks)])
    packed = slots * m + 2
    send, aux = pl.pallas_call(
        functools.partial(pair_kernel, slots=slots, copies=devices),
        in_specs=[smem, vmem, vmem],
        out_specs=[vmem, vmem],
        out_shape=[jax.ShapeDtypeStruct((devices, packed, LANES), F32), jax.ShapeDtypeStruct((SUBS, width), F32)],
        compiler_params=small,
        name="pair",
    )(place, totals, other)
    got = lax.all_to_all(send, ("tm", "env"), 0, 0, tiled=True)

    return tuple(pl.pallas_call(
        functools.partial(finish_kernel, slots=slots, pairs=pairs, groups=groups,
                          cells=1.0 * rows * width * devices),
        grid=(steps,),
        in_specs=[smem, vmem, vmem, vmem, vmem, vmem],
        out_specs=[fore, fore],
        out_shape=[full, full],
        scratch_shapes=[pltpu.VMEM((SUBS, width), F32), pltpu.VMEM((2, SUBS, LANES), F32)],
        compiler_params=small,
        name="finish",
    )(place, got, aux, level, gain, weight))


def solution(mesh):
    placed = (P("tm", "env"), P("tm", "env"), P("tm", "env"), P("env"), P("env"), P("env"))
    return jax.shard_map(
        local,
        mesh=mesh,
        in_specs=placed,
        out_specs=(P("tm", "env"), P("tm", "env")),
        check_vma=False,
    )
```

```python
import functools

import jax
import jax.numpy as jnp
from jax import lax
from jax.experimental import pallas as pl
from jax.experimental.pallas import tpu as pltpu
from jax.sharding import PartitionSpec as P

LANES = 128
SIDE = 1
SUBS = 8
F32 = jnp.float32


def spread(row):
    return jnp.broadcast_to(row, (SUBS, row.shape[1]))


def scan_kernel(r_hbm, v_hbm, d_hbm, boot_hbm, dh_hbm, th_hbm, g_ref, p_ref, v_ref, tot_ref,
                r_ref, d_ref, row_ref, carry, acc, sems, row_sems, *, part):
    rows, width = r_ref.shape
    count = rows // part
    row_copies = [pltpu.make_async_copy(x, row_ref.at[pl.ds(i, 1)], row_sems.at[i])
                  for i, x in enumerate((dh_hbm, th_hbm, boot_hbm))]
    for copy in row_copies:
        copy.start()

    def copies(n):
        at = pl.ds(pl.multiple_of(n * part, part), part)
        return [pltpu.make_async_copy(x.at[at], y.at[at], sems.at[i, n])
                for i, (x, y) in enumerate(((r_hbm, r_ref), (v_hbm, v_ref), (d_hbm, d_ref)))]

    for n in reversed(range(count)):
        for copy in copies(n):
            copy.start()
    carry[0] = jnp.zeros((SUBS, width), F32)
    carry[1] = jnp.ones((SUBS, width), F32)
    acc[...] = jnp.zeros(acc.shape, F32)
    sub = lax.broadcasted_iota(jnp.int32, (SUBS, LANES), 0)
    masks = {k: sub < SUBS - k for k in (1, 2, 4)}
    for copy in row_copies:
        copy.wait()

    def body(i, _):
        n = count - 1 - i
        for copy in copies(n):
            copy.wait()
        for first in range(0, width // LANES, SIDE):
            span = [pl.ds(c * LANES, LANES) for c in range(first, min(first + SIDE, width // LANES))]
            state = []
            for at in span:
                trace = 1.0 - 1.0 / row_ref[1:2, at]
                rate = (1.0 - 1.0 / row_ref[0:1, at]) * trace
                inv = 1.0 / trace
                state.append([spread(rate), spread(inv), spread(inv - 1.0), carry[0, :, at], carry[1, :, at],
                              [acc[i, :, at] for i in range(5)]])
            for j in reversed(range(part // SUBS)):
                rs = pl.ds(pl.multiple_of(n * part + j * SUBS, SUBS), SUBS)
                for b, at in enumerate(span):
                    rate, inv, extra, z_in, p_in, sums = state[b]
                    v = v_ref[rs, at]
                    u = r_ref[rs, at] + v * extra
                    a = jnp.where(d_ref[rs, at] != 0, 0.0, rate)
                    for k in (1, 2, 4):
                        m = masks[k]
                        u = u + jnp.where(m, a, 0.0) * pltpu.roll(u, SUBS - k, 0)
                        a = a * jnp.where(m, pltpu.roll(a, SUBS - k, 0), 1.0)
                    g = u + a * z_in - v * inv
                    p = a * p_in
                    z_in = spread(u[0:1]) + spread(a[0:1]) * z_in
                    p_in = spread(a[0:1]) * p_in
                    g_ref[rs, at] = g
                    p_ref[rs, at] = p
                    sums = [sums[0] + p, sums[1] + g * p, sums[2] + p * p, sums[3] + g, sums[4] + g * g]
                    state[b] = [rate, inv, extra, z_in, p_in, sums]
            for at, (_, _, _, z_in, p_in, sums) in zip(span, state):
                carry[0, :, at] = z_in
                carry[1, :, at] = p_in
                for i in range(5):
                    acc[i, :, at] = sums[i]
        return 0

    lax.fori_loop(0, count, body, 0)
    tot_ref[0:1] = carry[1, 0:1]
    tot_ref[1:2] = carry[0, 0:1]
    for i in range(5):
        tot_ref[2 + i:3 + i] = jnp.sum(acc[i], axis=0, keepdims=True)
    tot_ref[7:8] = row_ref[2:3] / (1.0 - 1.0 / row_ref[1:2])


def pair_kernel(at_ref, mine_ref, other_ref, send_ref, aux_ref, *, slots, copies):
    width = mine_ref.shape[1]
    half = width // 2
    m = half // LANES
    odd, last = at_ref[0], at_ref[1]
    late_here = odd == 1
    mine, other = mine_ref[...], other_ref[...]
    late = jnp.where(late_here, mine, other)
    early = jnp.where(late_here, other, mine)
    la, lz, lp, lgp, lpp, lg, lgg = [late[i:i + 1] for i in range(7)]
    ea, ez, ep, egp, epp, eg, egg = [early[i:i + 1] for i in range(7)]
    a, z = la * ea, ez + ea * lz
    p = lp + ep * la
    gp = lgp + (egp + epp * lz) * la
    pp = lpp + epp * la * la
    g = lg + eg + ep * lz
    gg = lgg + egg + (2.0 * egp + epp * lz) * lz
    known = mine[7:8]
    is_last = last == 1
    g_end = g + p * known
    gg_end = gg + (2.0 * gp + pp * known) * known
    z_end = z + a * known
    g = jnp.where(is_last, g_end, g)
    gg = jnp.where(is_last, gg_end, gg)
    if slots == 3:
        parts = [jnp.where(is_last, z_end, p), gp, pp]
    else:
        parts = [jnp.where(is_last, z_end, z), p, gp, pp, a]
    mult = jnp.where(late_here, jnp.ones_like(la), la)
    add = jnp.where(late_here, jnp.zeros_like(la), lz)
    aux_ref[0:1] = jnp.where(is_last, 0.0, mult)
    aux_ref[1:2] = jnp.where(is_last, add + mult * known, add)
    aux_ref[2:8] = jnp.zeros((6, width), F32)

    def own(x):
        return jnp.where(late_here, x[:, half:], x[:, :half])

    rows = []
    for part in parts:
        h = own(part)
        rows += [h[:, i * LANES:(i + 1) * LANES] for i in range(m)]
    for total in (g, gg):
        h = own(total)
        rows.append(sum(h[:, i * LANES:(i + 1) * LANES] for i in range(m)))
    block = jnp.concatenate(rows, axis=0)
    send_ref[...] = jnp.broadcast_to(block[None], (copies,) + block.shape)


def finish_kernel(at_ref, got_ref, aux_ref, v_ref, g_ref, p_ref, norm_hbm, ret_hbm, norm_ref, ret_ref, sems,
                  *, slots, pairs, groups, cells, part):
    rows, width = norm_ref.shape
    half = width // 2
    m = half // LANES
    count = rows // part

    pair, group = at_ref[2], at_ref[3]
    n = 2 * groups
    base = slots * m
    got = [got_ref[k * n:(k + 1) * n] for k in range(pairs)]
    s1 = sum(jnp.sum(x[:, base:base + 1], axis=0) for x in got)
    s2 = sum(jnp.sum(x[:, base + 1:base + 2], axis=0) for x in got)
    off = 0 if slots == 3 else m
    z = got[pairs - 1][:, 0:m]
    here = [got_ref[(pairs - 1) * n + core * groups + group, 0:m] for core in range(2)]
    pick = here
    for k in reversed(range(pairs - 1)):
        x = got[k]
        p, gp, pp = [x[:, off + i * m:off + (i + 1) * m] for i in range(3)]
        t1 = jnp.sum(p * z, axis=0)
        t2 = jnp.sum((2.0 * gp + pp * z) * z, axis=0)
        s1 = s1 + jnp.sum(t1, axis=0, keepdims=True)
        s2 = s2 + jnp.sum(t2, axis=0, keepdims=True)
        pick = [jnp.where(pair == k, b, a) for a, b in zip(pick, here)]
        if k:
            z = x[:, 0:m] + x[:, 4 * m:5 * m] * z
            nxt = [got_ref[k * n + core * groups + group] for core in range(2)]
            here = [y[0:m] + y[4 * m:5 * m] * h for y, h in zip(nxt, here)]
    flat = jnp.concatenate([h[i:i + 1] for h in pick for i in range(m)], axis=1)
    z_in = aux_ref[1:2] + aux_ref[0:1] * flat
    mean = jnp.sum(s1, axis=1, keepdims=True) / cells
    var = jnp.sum(s2, axis=1, keepdims=True) / cells - mean * mean
    scale = 1.0 / jnp.sqrt(var + 1.0)
    mean = jnp.broadcast_to(mean, (SUBS, LANES))
    scale = jnp.broadcast_to(scale, (SUBS, LANES))

    def copy(n, i):
        at = pl.ds(n * part, part)
        x, y = ((ret_ref, ret_hbm), (norm_ref, norm_hbm))[i]
        return pltpu.make_async_copy(x.at[at], y.at[at], sems.at[i, n])

    def tiles(n):
        for c in range(width // LANES):
            at = pl.ds(c * LANES, LANES)
            z = spread(z_in[:, c * LANES:(c + 1) * LANES])
            for j in range(part // SUBS):
                rs = pl.ds(n * part + j * SUBS, SUBS)
                yield rs, at, g_ref[rs, at] + p_ref[rs, at] * z

    for n in range(count):
        for rs, at, adv in tiles(n):
            ret_ref[rs, at] = adv + v_ref[rs, at]
        copy(n, 0).start()
    for n in range(count):
        for rs, at, adv in tiles(n):
            norm_ref[rs, at] = (adv - mean) * scale
        copy(n, 1).start()
    for n in range(count):
        copy(n, 0).wait()
    for n in range(count):
        copy(n, 1).wait()


def local(rewards, values, done_flags, bootstrap, discount_horizon, trace_horizon):
    rows, width = rewards.shape
    blocks, groups = lax.axis_size("tm"), lax.axis_size("env")
    pairs, devices = blocks // 2, blocks * groups
    slots = 3 if pairs == 2 else 5
    m = width // 2 // LANES
    block_at, group = lax.axis_index("tm"), lax.axis_index("env")
    place = jnp.stack([block_at % 2, (block_at // 2 == pairs - 1).astype(jnp.int32), block_at // 2, group]).astype(jnp.int32)
    boot, dh, th = bootstrap[None], discount_horizon[None], trace_horizon[None]

    part = max(SUBS, rows // 2)
    count = rows // part
    out_part = max(SUBS, rows // 4)
    vmem = pl.BlockSpec(memory_space=pltpu.VMEM)
    smem = pl.BlockSpec(memory_space=pltpu.SMEM)
    hbm = pl.BlockSpec(memory_space=pltpu.HBM)
    small = pltpu.CompilerParams(vmem_limit_bytes=16 << 20)
    full = jax.ShapeDtypeStruct((rows, width), F32)
    gain, weight, kept, totals = pl.pallas_call(
        functools.partial(scan_kernel, part=part),
        in_specs=[hbm] * 6,
        out_specs=[vmem] * 4,
        out_shape=[full, full, full, jax.ShapeDtypeStruct((SUBS, width), F32)],
        scratch_shapes=[
            pltpu.VMEM((rows, width), F32), pltpu.VMEM((rows, width), jnp.int32), pltpu.VMEM((SUBS, width), F32),
            pltpu.VMEM((2, SUBS, width), F32), pltpu.VMEM((5, SUBS, width), F32),
            pltpu.SemaphoreType.DMA((3, count)), pltpu.SemaphoreType.DMA((3,)),
        ],
        compiler_params=small,
        name="scan",
    )(*(pltpu.with_memory_space_constraint(x, pltpu.HBM)
        for x in (rewards, values, done_flags, boot, dh, th)))

    other = lax.ppermute(totals, "tm", [(i, i ^ 1) for i in range(blocks)])
    packed = slots * m + 2
    send, aux = pl.pallas_call(
        functools.partial(pair_kernel, slots=slots, copies=devices),
        in_specs=[smem, vmem, vmem],
        out_specs=[vmem, vmem],
        out_shape=[jax.ShapeDtypeStruct((devices, packed, LANES), F32), jax.ShapeDtypeStruct((SUBS, width), F32)],
        compiler_params=small,
        name="pair",
    )(place, totals, other)
    got = lax.all_to_all(send, ("tm", "env"), 0, 0, tiled=True)

    return tuple(pl.pallas_call(
        functools.partial(finish_kernel, slots=slots, pairs=pairs, groups=groups,
                          cells=1.0 * rows * width * devices, part=out_part),
        in_specs=[smem, vmem, vmem, vmem, vmem, vmem],
        out_specs=[hbm, hbm],
        out_shape=[full, full],
        scratch_shapes=[pltpu.VMEM((rows, width), F32), pltpu.VMEM((rows, width), F32),
                        pltpu.SemaphoreType.DMA((2, rows // out_part))],
        compiler_params=small,
        name="finish",
    )(place, got, aux, kept, gain, weight))


def solution(mesh):
    placed = (P("tm", "env"), P("tm", "env"), P("tm", "env"), P("env"), P("env"), P("env"))
    return jax.shard_map(
        local,
        mesh=mesh,
        in_specs=placed,
        out_specs=(P("tm", "env"), P("tm", "env")),
        check_vma=False,
    )
```
